128 devices in a mesh: member: 1, lon: 16 (over z, y), lat: 8 (over x, core).
Axes of the slice: x: 4, y: 4, z: 4, core: 2. Of those that a mesh axis runs over, the one named last changes fastest.
Arguments:
- field_in: float32 [8, 256, 192, 384], P('member', None, 'lat', 'lon')
- fwd_table: float32 [128, 128, 192], replicated
- inv_table: float32 [128, 128, 192], replicated
- mix_weights: float32 [128, 256, 256, 2], replicated
Outputs:
- output: float32 [8, 256, 192, 384], P('member', None, 'lat', 'lon')
All inputs are finite; a program needn't handle non-finite values.
Results may differ from the reference program's by a relative error of at most 0.00401796.
Values are sent between devices in bfloat16 or wider.
A program may use at most 1 GiB of HBM per device.

```python
import math
import jax
import jax.numpy as jnp
from jax import lax

SAMPLES = 8
CHANNELS = 256
LATITUDES = 192
DEGREES = 128
LONGITUDES = 2 * LATITUDES


def as_bf16(values):
    return values.astype(jnp.bfloat16).astype(jnp.float32)


def legendre_table(colatitude):
    cos_t = jnp.cos(colatitude)
    log_sin = jnp.log(jnp.sin(colatitude))
    orders = jnp.arange(DEGREES).astype(jnp.float32)
    log_steps = jnp.cumsum(jnp.log((2.0 * orders + 1.0) / (2.0 * orders + 2.0)))
    log_prod = jnp.concatenate([jnp.zeros((1,), jnp.float32), log_steps[:-1]])
    log_diag = 0.5 * (jnp.log((2.0 * orders + 1.0) / (4.0 * math.pi)) + log_prod)
    diag_vals = jnp.exp(log_diag[:, None] + orders[:, None] * log_sin[None, :])

    def degree_step(carry_vals, degree):
        prev_two, prev_one = carry_vals
        deg_f = degree.astype(jnp.float32)
        coef_a = jnp.sqrt(jnp.maximum(4.0 * deg_f * deg_f - 1.0, 0.0) / jnp.maximum(deg_f * deg_f - orders * orders, 1.0))
        prev_f = deg_f - 1.0
        coef_b = jnp.sqrt(jnp.maximum(prev_f * prev_f - orders * orders, 0.0) / jnp.maximum(4.0 * prev_f * prev_f - 1.0, 1.0))
        recur_val = coef_a[:, None] * (cos_t[None, :] * prev_one - coef_b[:, None] * prev_two)
        next_val = jnp.where((deg_f == orders)[:, None], diag_vals, jnp.where((deg_f > orders)[:, None], recur_val, 0.0))
        return (prev_one, next_val), next_val

    zero_rows = jnp.zeros((DEGREES, LATITUDES), jnp.float32)
    _, leg_table = lax.scan(degree_step, (zero_rows, zero_rows), jnp.arange(DEGREES))
    return jnp.transpose(leg_table, (1, 0, 2))


def setup_inputs(seed: int = 0, part: int = 0) -> dict:
    root_key = jax.random.key(seed)
    key_field, key_fwd, key_inv, key_mix = jax.random.split(root_key, 4)
    key_part = jax.random.fold_in(key_field, part)
    key_noise, key_smooth = jax.random.split(key_part, 2)
    colatitude = math.pi * (jnp.arange(LATITUDES).astype(jnp.float32) + 0.5) / LATITUDES
    longitude = (2.0 * math.pi / LONGITUDES) * jnp.arange(LONGITUDES).astype(jnp.float32)
    smooth_coef = jax.random.normal(key_smooth, (SAMPLES, CHANNELS, 3, 1, 1), jnp.float32)
    smooth = smooth_coef[:, :, 0] * jnp.cos(colatitude)[:, None] + jnp.sin(colatitude)[:, None] * (smooth_coef[:, :, 1] * jnp.cos(longitude) + smooth_coef[:, :, 2] * jnp.sin(longitude))
    white_noise = jax.random.normal(key_noise, (SAMPLES, CHANNELS, LATITUDES, LONGITUDES), jnp.float32)
    field_in = smooth + white_noise
    leg_table = legendre_table(colatitude)
    quad_weights = (2.0 * math.pi / LONGITUDES) * (math.pi / LATITUDES) * jnp.sin(colatitude)
    table_shape = (DEGREES, DEGREES, LATITUDES)
    fwd_table = leg_table * quad_weights * (1.0 + 0.3 * jax.random.uniform(key_fwd, table_shape, jnp.float32, -1.0, 1.0))
    inv_table = leg_table * (1.0 + 0.3 * jax.random.uniform(key_inv, table_shape, jnp.float32, -1.0, 1.0))
    mix_scale = LATITUDES / (DEGREES * math.sqrt(CHANNELS))
    mix_weights = mix_scale * jax.random.normal(key_mix, (DEGREES, CHANNELS, CHANNELS, 2), jnp.float32)
    return {'field_in': field_in, 'fwd_table': fwd_table, 'inv_table': inv_table, 'mix_weights': mix_weights}


def reference(field_in, fwd_table, inv_table, mix_weights):
    lon_ids = jnp.arange(LONGITUDES)
    wave_ids = jnp.arange(DEGREES)
    phase_arg = (2.0 * math.pi / LONGITUDES) * ((lon_ids[:, None] * wave_ids[None, :]) % LONGITUDES).astype(jnp.float32)
    weight_m = jnp.where(wave_ids == 0, 1.0, 2.0).astype(jnp.float32)
    cos_fwd = as_bf16(jnp.cos(phase_arg))
    sin_fwd = as_bf16(-jnp.sin(phase_arg))
    cos_inv = as_bf16(weight_m * jnp.cos(phase_arg))
    sin_inv = as_bf16(-weight_m * jnp.sin(phase_arg))
    fwd_bf = as_bf16(fwd_table)
    inv_bf = as_bf16(inv_table)
    w_re = as_bf16(mix_weights[..., 0])
    w_im = as_bf16(mix_weights[..., 1])

    def one_sample(sample):
        grid_val = as_bf16(sample)
        spec_re = as_bf16(jnp.einsum('ctj,jm->ctm', grid_val, cos_fwd))
        spec_im = as_bf16(jnp.einsum('ctj,jm->ctm', grid_val, sin_fwd))
        coef_re = as_bf16(jnp.einsum('mlt,ctm->clm', fwd_bf, spec_re))
        coef_im = as_bf16(jnp.einsum('mlt,ctm->clm', fwd_bf, spec_im))
        mixed_re = as_bf16(jnp.einsum('loi,ilm->olm', w_re, coef_re) - jnp.einsum('loi,ilm->olm', w_im, coef_im))
        mixed_im = as_bf16(jnp.einsum('loi,ilm->olm', w_re, coef_im) + jnp.einsum('loi,ilm->olm', w_im, coef_re))
        back_re = as_bf16(jnp.einsum('mlt,clm->ctm', inv_bf, mixed_re))
        back_im = as_bf16(jnp.einsum('mlt,clm->ctm', inv_bf, mixed_im))
        wave_grid = as_bf16(jnp.einsum('ctm,jm->ctj', back_re, cos_inv) + jnp.einsum('ctm,jm->ctj', back_im, sin_inv))
        return sample + jax.nn.gelu(wave_grid, approximate=True)

    return lax.map(one_sample, field_in)
```

```python
import math
import numpy as np
import jax
import jax.numpy as jnp
from jax import lax
from jax.experimental import pallas as pl
from jax.experimental.pallas import tpu as pltpu
from jax.sharding import PartitionSpec as P

MESH = pl.DeviceIdType.MESH
F32 = jnp.float32
BF16 = jnp.bfloat16

SAMPLES = 8
LON = 16
LAT = 8
ROWS = 576
CHUNK_T = 4
CHUNKS = 6
CROWS = CHUNK_T * 24
TS = 40
LS = 24
W_SLOTS = 8

PEERS = [(2, 2), (2, 1), (2, 3), (1, 2), (3, 2), (2, 0), (0, 2), (1, 1), (3, 3), (1, 3), (3, 1), (1, 0), (0, 1), (3, 0), (0, 3)]


def dft_matrices():
    lon_ids = np.arange(384)
    waves = np.arange(128)
    phase = np.float32(2.0 * math.pi / 384) * ((lon_ids[:, None] * waves[None, :]) % 384).astype(np.float32)
    cos_val, sin_val = np.cos(phase), np.sin(phase)
    weight = np.where(waves == 0, 1.0, 2.0).astype(np.float32)
    fwd = np.stack([cos_val, -sin_val])
    inv = np.stack([weight * cos_val, -weight * sin_val])
    out = []
    for tab in (fwd, inv):
        tab = tab.reshape(2, 16, 24, 16, 8)
        full = np.zeros((8, 2, 2, 16, 16, 2, 24), np.float32)
        part = tab.transpose(4, 0, 3, 1, 2)
        for tt in range(2):
            full[:, tt, :, :, :, tt, :] = part
        out.append(full.reshape(512, 768))
    return out[0].astype(jnp.bfloat16), np.ascontiguousarray(out[1].T).astype(jnp.bfloat16)


def kernel(x_hbm, ft_hbm, it_hbm, w_hbm, dfwd, dinv, y_hbm,
           xf, xs, ra, sp, rb, t1, cf, rc, t2, wb, ws, fs, gs, fb, ib, t3, sd, rd, s2, rebuf, ys,
           x_sem, tab_sem, w_sem, a_send, a_recv, b_send, b_recv, c_send, c_recv, d_send, d_recv,
           e_send, e_recv, f_send, f_recv):
    lon = lax.axis_index('lon')
    lat = lax.axis_index('lat')
    half = lax.rem(lon, 2)
    core = lax.rem(lat, 2)
    quarter = 2 * half + core
    sample = lon // 2

    def dev(n, t):
        return dict(device_id=(0, n, t), device_id_type=MESH)

    def lon_peer(dz, dy):
        return lax.rem(lon // 4 + dz, 4) * 4 + lax.rem(lax.rem(lon, 4) + dy, 4)

    def lat_peer(d):
        return lax.rem(lat + d, LAT)

    def quad(tq):
        return (lon // 2) * 2 + tq // 2, (lat // 2) * 2 + tq % 2

    def rows(ch, size=CROWS, off=0):
        return pl.ds(pl.multiple_of(ch * CROWS + off, 16), size)

    lanes_half = pl.ds(pl.multiple_of(half * 128, 128), 128)

    for ch in range(CHUNKS):
        pltpu.make_async_copy(x_hbm.at[:, pl.ds(ch * CROWS, CROWS)], xf.at[:, pl.ds(ch * CROWS, CROWS)], x_sem.at[ch]).start()
    fwd_load = pltpu.make_async_copy(ft_hbm.at[:, lat], fs, tab_sem.at[0])
    inv_load = pltpu.make_async_copy(it_hbm.at[:, lat], gs, tab_sem.at[1])
    fwd_load.start()
    inv_load.start()

    def degree(idx):
        return jnp.where(idx < 16, quarter * 16 + idx, (7 - quarter) * 16 + idx - 16)

    def w_load(idx):
        slot = lax.rem(idx, W_SLOTS)
        return pltpu.make_async_copy(w_hbm.at[degree(idx)], ws.at[slot], w_sem.at[slot])

    for idx in range(W_SLOTS):
        w_load(jnp.int32(idx)).start()

    rc[...] = jnp.zeros_like(rc)
    rd[...] = jnp.zeros_like(rd)

    bar = pltpu.get_barrier_semaphore()
    for dz, dy in PEERS:
        pl.semaphore_signal(bar, inc=1, **dev(lon_peer(dz, dy), lat))
    for d in range(1, LAT):
        pl.semaphore_signal(bar, inc=1, **dev(lon, lat_peer(d)))
    pl.semaphore_signal(bar, inc=1, **dev((lon // 2) * 2 + 1 - half, (lat // 2) * 2 + 1 - core))
    pl.semaphore_wait(bar, 15 + 7 + 1)

    def send_a(ch, _):
        pltpu.make_async_copy(xf.at[:, rows(ch)], xf.at[:, rows(ch)], x_sem.at[ch]).wait()
        for s in range(SAMPLES):
            for h in range(2):
                xs[2 * s + h, rows(ch), :] = xf[s, rows(ch), h * 128:(h + 1) * 128].astype(BF16)
        for dz, dy in PEERS:
            peer = lon_peer(dz, dy)
            pltpu.make_async_remote_copy(xs.at[peer, rows(ch)], ra.at[lon, rows(ch)], a_send.at[ch], a_recv.at[ch],
                                         **dev(peer, lat)).start()
        pltpu.make_async_copy(xs.at[lon, rows(ch)], ra.at[lon, rows(ch)], a_recv.at[ch]).start()
        return 0

    lax.fori_loop(0, CHUNKS, send_a, 0)

    fwd_load.wait()
    inv_load.wait()

    def prep_tables(i, _):
        fb[i] = fs[i].T.astype(BF16)
        ib[i] = gs[i].astype(BF16)
        return 0

    lax.fori_loop(0, 16, prep_tables, 0)

    def prep_weights(idx, _):
        w_load(idx).wait()
        slot = lax.rem(idx, W_SLOTS)
        for ri in range(2):
            for it in range(2):
                wb[idx, :, ri * 256 + it * 128: ri * 256 + (it + 1) * 128] = ws[slot, pl.ds(2 * it + ri, 256, stride=4), :].astype(BF16)

        @pl.when(idx + W_SLOTS < 32)
        def _():
            w_load(idx + W_SLOTS).start()

        return 0

    def take_b(ch):
        chunk = pl.ds(ch * CHUNK_T, CHUNK_T)
        pltpu.make_async_copy(rb.at[:, chunk], rb.at[:, chunk], b_recv.at[ch]).wait()

        def one(kk, _):
            for tt in range(CHUNK_T):
                row = pl.multiple_of((kk * 24 + ch * CHUNK_T + tt) * TS, 8)
                t1[pl.ds(row, 32), :] = rb[kk, ch * CHUNK_T + tt].astype(F32)
            return 0

        lax.fori_loop(0, LAT, one, 0)

    def dft(ch, _):
        lax.fori_loop(ch * 6, jnp.minimum(ch * 6 + 6, 32), prep_weights, 0)
        pltpu.make_async_copy(ra.at[:, rows(ch)], ra.at[:, rows(ch)], a_recv.at[ch]).wait()
        rhs = jnp.concatenate([ra[:, rows(ch, 48, a * 48), :].reshape(768, 128) for a in range(2)], axis=1)
        out = jnp.dot(dfwd[...], rhs, preferred_element_type=F32)
        for a in range(2):
            sp[:, pl.ds(ch * CHUNK_T + 2 * a, 2)] = out[:, a * 128:(a + 1) * 128].astype(BF16).reshape(8, 2, 32, 128)
        chunk = pl.ds(ch * CHUNK_T, CHUNK_T)
        for d in range(1, LAT):
            peer = lat_peer(d)
            pltpu.make_async_remote_copy(sp.at[peer, chunk], rb.at[lat, chunk], b_send.at[ch], b_recv.at[ch],
                                         **dev(lon, peer)).start()
        pltpu.make_async_copy(sp.at[lat, chunk], rb.at[lat, chunk], b_recv.at[ch]).start()

        @pl.when(ch > 0)
        def _():
            take_b(ch - 1)

        return 0

    lax.fori_loop(0, CHUNKS, dft, 0)
    take_b(CHUNKS - 1)

    def legendre(i, _):
        rhs = jnp.concatenate([t1[pl.ds(i, 192, stride=TS), :], t1[pl.ds(16 + i, 192, stride=TS), :]], axis=1).astype(BF16)
        cf[i] = jnp.dot(fb[i], rhs, preferred_element_type=F32).astype(BF16)
        return 0

    lax.fori_loop(0, 16, legendre, 0, unroll=4)

    for b in range(7, -1, -1):
        tq, lohi, n = (b, 0, 2 * b + 2) if b < 4 else (7 - b, 1, 2 * b + 2)
        src = cf.at[pl.ds(0, n), pl.ds(16 * b, 16)]
        dst = rc.at[pl.ds((quarter * 2 + lohi) * 16, n)]

        @pl.when(quarter == tq)
        def _():
            pltpu.make_async_copy(src, dst, c_recv).start()

        @pl.when(quarter != tq)
        def _():
            pltpu.make_async_remote_copy(src, dst, c_send, c_recv, **dev(*quad(tq))).start()

    pltpu.make_async_copy(rc.at[pl.ds(0, 72)], rc.at[pl.ds(0, 72)], c_recv).wait()

    def take_c(u, _):
        for ri in range(2):
            t2[ri, pl.ds(pl.multiple_of(u * LS, 8), 16), :] = rc[u, :, ri * 128:(ri + 1) * 128].astype(F32)
        return 0

    lax.fori_loop(0, 128, take_c, 0, unroll=4)

    def mix(idx, lohi):
        r = idx - lohi * 16

        def part(ri):
            return jnp.concatenate([jnp.concatenate([
                t2[ri, pl.ds(((2 * hs + cs) * 2 + lohi) * 16 * LS + r, 16, stride=LS), :] for hs in range(2)], axis=1)
                for cs in range(2)], axis=0)

        re, im = part(0), part(1)
        lhs = jnp.concatenate([jnp.concatenate([re, -im], axis=1), jnp.concatenate([im, re], axis=1)], axis=0).astype(BF16)
        out = lax.dot_general(lhs, wb[idx], (((1,), (1,)), ((), ())), preferred_element_type=F32)
        for ri in range(2):
            for oh in range(2):
                t3[ri * 2 + oh, pl.ds(lohi * 32 * LS + r, 32, stride=LS), :] = out[ri * 32:(ri + 1) * 32, oh * 128:(oh + 1) * 128]

    for lohi in (1, 0):
        def mix_step(idx, _, lohi=lohi):
            mix(idx, lohi)
            return 0

        lax.fori_loop(lohi * 16, lohi * 16 + 16, mix_step, 0, unroll=4)

        def pack_d(i, _, lohi=lohi):
            for oh in range(2):
                for cs in range(2):
                    for ri in range(2):
                        row = pl.multiple_of(lohi * 32 * LS + (cs * 16 + i) * LS, 8)
                        sd[((oh * 2 + cs) * 2 + lohi) * 16 + i, :, ri * 128:(ri + 1) * 128] = t3[ri * 2 + oh, pl.ds(row, 16), :].astype(BF16)
            return 0

        lax.fori_loop(0, 16, pack_d, 0)

        for qq in range(4):
            b = qq if lohi == 0 else 7 - qq
            n = 2 * b + 2

            @pl.when(quarter == qq)
            def _():
                for tq in range(4):
                    src = sd.at[pl.ds((tq * 2 + lohi) * 16, n)]
                    dst = rd.at[pl.ds(0, n), pl.ds(16 * b, 16)]
                    if tq == qq:
                        pltpu.make_async_copy(src, dst, d_recv).start()
                    else:
                        pltpu.make_async_remote_copy(src, dst, d_send, d_recv, **dev(*quad(tq))).start()

    pltpu.make_async_copy(rc.at[pl.ds(0, 72)], rc.at[pl.ds(0, 72)], d_recv).wait()

    def inverse(i, _):
        out = jnp.dot(ib[i], rd[i], preferred_element_type=F32)
        t1[pl.ds(i, 192, stride=TS), :] = out[:, :128]
        t1[pl.ds(16 + i, 192, stride=TS), :] = out[:, 128:]
        return 0

    lax.fori_loop(0, 16, inverse, 0, unroll=4)

    def send_e(ch, _):
        chunk = pl.ds(ch * CHUNK_T, CHUNK_T)

        def one(kk, _):
            for tt in range(CHUNK_T):
                row = pl.multiple_of((kk * 24 + ch * CHUNK_T + tt) * TS, 8)
                s2[kk, ch * CHUNK_T + tt] = t1[pl.ds(row, 32), :].astype(BF16)
            return 0

        lax.fori_loop(0, LAT, one, 0)
        for d in range(1, LAT):
            peer = lat_peer(d)
            pltpu.make_async_remote_copy(s2.at[peer, chunk], rebuf.at[lat, chunk], e_send.at[ch], e_recv.at[ch],
                                         **dev(lon, peer)).start()
        pltpu.make_async_copy(s2.at[lat, chunk], rebuf.at[lat, chunk], e_recv.at[ch]).start()
        return 0

    lax.fori_loop(0, CHUNKS, send_e, 0)

    def idft(ch, _):
        chunk = pl.ds(ch * CHUNK_T, CHUNK_T)
        pltpu.make_async_copy(rebuf.at[:, chunk], rebuf.at[:, chunk], e_recv.at[ch]).wait()
        rhs = jnp.concatenate([rebuf[:, pl.ds(ch * CHUNK_T + 2 * a, 2)].reshape(512, 128) for a in range(2)], axis=1)
        out = jnp.dot(dinv[...], rhs, preferred_element_type=F32)
        for a in range(2):
            ys[:, rows(ch, 48, a * 48), :] = out[:, a * 128:(a + 1) * 128].astype(BF16).reshape(16, 48, 128)
        for dz, dy in PEERS:
            peer = lon_peer(dz, dy)
            pltpu.make_async_remote_copy(ys.at[peer, rows(ch)], y_hbm.at[sample, rows(ch), lanes_half], f_send, f_recv,
                                         **dev(peer, lat)).start()
        pltpu.make_async_copy(ys.at[lon, rows(ch)], y_hbm.at[sample, rows(ch), lanes_half], f_recv).start()
        return 0

    lax.fori_loop(0, CHUNKS, idft, 0)

    def drain(ch, _):
        chunk = pl.ds(ch * CHUNK_T, CHUNK_T)
        pltpu.make_async_copy(xs.at[pl.ds(0, 15), rows(ch)], xs.at[pl.ds(0, 15), rows(ch)], a_send.at[ch]).wait()
        pltpu.make_async_copy(sp.at[pl.ds(0, 7), chunk], sp.at[pl.ds(0, 7), chunk], b_send.at[ch]).wait()
        pltpu.make_async_copy(s2.at[pl.ds(0, 7), chunk], s2.at[pl.ds(0, 7), chunk], e_send.at[ch]).wait()
        return 0

    lax.fori_loop(0, CHUNKS, drain, 0)
    for tq in range(4):
        @pl.when(quarter == tq)
        def _():
            n = 72 - 18
            pltpu.make_async_copy(rc.at[pl.ds(0, n)], rc.at[pl.ds(0, n)], c_send).wait()
            pltpu.make_async_copy(rc.at[pl.ds(0, n)], rc.at[pl.ds(0, n)], d_send).wait()
    pltpu.make_async_copy(ys.at[pl.ds(0, 15)], ys.at[pl.ds(0, 15)], f_send).wait()
    pltpu.make_async_copy(y_hbm, y_hbm, f_recv).wait()


def solution(mesh):
    grid_spec = P('member', None, 'lat', 'lon')
    dfwd, dinv = dft_matrices()

    def local_layer(field_in, fwd_table, inv_table, mix_weights):
        rows_view = field_in.transpose(0, 2, 3, 1).reshape(SAMPLES, ROWS, 256)
        ft = fwd_table.transpose(0, 2, 1).reshape(16, 8, 192, 128)
        it = inv_table.transpose(0, 2, 1).reshape(16, 8, 192, 128)
        w = mix_weights.reshape(128, 256, 2, 128, 2).transpose(0, 1, 2, 4, 3).reshape(128, 1024, 128)
        dma = pltpu.SemaphoreType.DMA
        y = pl.pallas_call(
            kernel,
            out_shape=jax.ShapeDtypeStruct((SAMPLES, ROWS, 256), BF16),
            in_specs=[pl.BlockSpec(memory_space=pl.ANY)] * 4 + [pl.BlockSpec(memory_space=pltpu.VMEM)] * 2,
            out_specs=pl.BlockSpec(memory_space=pl.ANY),
            scratch_shapes=[
                pltpu.VMEM((SAMPLES, ROWS, 256), F32),
                pltpu.VMEM((LON, ROWS, 128), BF16),
                pltpu.VMEM((LON, ROWS, 128), BF16),
                pltpu.VMEM((LAT, 24, 32, 128), BF16),
                pltpu.VMEM((LAT, 24, 32, 128), BF16),
                pltpu.VMEM((192 * TS, 128), F32),
                pltpu.VMEM((16, 128, 256), BF16),
                pltpu.VMEM((128, 16, 256), BF16),
                pltpu.VMEM((2, 128 * LS, 128), F32),
                pltpu.VMEM((32, 256, 512), BF16),
                pltpu.VMEM((W_SLOTS, 1024, 128), F32),
                pltpu.VMEM((16, 192, 128), F32),
                pltpu.VMEM((16, 192, 128), F32),
                pltpu.VMEM((16, 128, 192), BF16),
                pltpu.VMEM((16, 192, 128), BF16),
                pltpu.VMEM((4, 64 * LS, 128), F32),
                pltpu.VMEM((128, 16, 256), BF16),
                pltpu.VMEM((16, 128, 256), BF16),
                pltpu.VMEM((LAT, 24, 32, 128), BF16),
                pltpu.VMEM((LAT, 24, 32, 128), BF16),
                pltpu.VMEM((LON, ROWS, 128), BF16),
                dma((CHUNKS,)), dma((2,)), dma((W_SLOTS,)),
                dma((CHUNKS,)), dma((CHUNKS,)), dma((CHUNKS,)), dma((CHUNKS,)),
                dma, dma, dma, dma,
                dma((CHUNKS,)), dma((CHUNKS,)), dma, dma,
            ],
            compiler_params=pltpu.CompilerParams(collective_id=0, has_side_effects=True, vmem_limit_bytes=67043328),
        )(rows_view, ft, it, w, jnp.asarray(dfwd), jnp.asarray(dinv))
        y = y.reshape(SAMPLES, 24, 24, 256).transpose(0, 3, 1, 2)
        return field_in + jax.nn.gelu(y.astype(F32), approximate=True)

    return jax.shard_map(local_layer, mesh=mesh, in_specs=(grid_spec, P(), P(), P()), out_specs=grid_spec, check_vma=False)
```

```python
import math
import numpy as np
import jax
import jax.numpy as jnp
from jax import lax
from jax.experimental import pallas as pl
from jax.experimental.pallas import tpu as pltpu
from jax.sharding import PartitionSpec as P

MESH = pl.DeviceIdType.MESH
F32 = jnp.float32
BF16 = jnp.bfloat16

SAMPLES = 8
LON = 16
LAT = 8
ROWS = 576
CHUNK_T = 2
CHUNKS = 12
CROWS = CHUNK_T * 24
TS = 40
LS = 24
W_SLOTS = 8

EVEN = [(2, 2), (1, 1), (3, 3), (1, 3), (3, 1), (2, 0), (0, 2), (0, 0)]
PEERS = [(2, 2), (2, 1), (2, 3), (1, 2), (3, 2), (2, 0), (0, 2), (1, 1), (3, 3), (1, 3), (3, 1), (1, 0), (0, 1), (3, 0), (0, 3)]


def dft_matrices():
    lon_ids = np.arange(384)
    waves = np.arange(128)
    phase = np.float32(2.0 * math.pi / 384) * ((lon_ids[:, None] * waves[None, :]) % 384).astype(np.float32)
    cos_val, sin_val = np.cos(phase), np.sin(phase)
    weight = np.where(waves == 0, 1.0, 2.0).astype(np.float32)
    fwd = np.stack([cos_val, -sin_val])
    inv = np.stack([weight * cos_val, -weight * sin_val])
    out = []
    for tab in (fwd, inv):
        tab = tab.reshape(2, 16, 24, 16, 8)
        full = np.zeros((8, 2, 2, 16, 16, 2, 24), np.float32)
        part = tab.transpose(4, 0, 3, 1, 2)
        for tt in range(2):
            full[:, tt, :, :, :, tt, :] = part
        out.append(full.reshape(512, 768))
    return out[0].astype(jnp.bfloat16), np.ascontiguousarray(out[1].T).astype(jnp.bfloat16)


def kernel(x_hbm, ft_hbm, it_hbm, w_hbm, dfwd, dinv, o_hbm,
           xf, xs, ra, sp, rb, t1, cf, rc, t2, wb, ws, fs, gs, fb, ib, t3, sd, rd, s2, rebuf, ys, yr,
           x_sem, tab_sem, w_sem, a_send, a_recv, b_send, b_recv, c_send, c_recv, d_send, d_recv,
           e_send, e_recv, f_send, f_recv, o_sem):
    lon = lax.axis_index('lon')
    lat = lax.axis_index('lat')
    z, y = lon // 4, lax.rem(lon, 4)
    group = lax.rem(z + y, 2)
    sample = group * 4 + z
    half = y // 2
    core = lax.rem(lat, 2)
    quarter = 2 * half + core

    def dev(n, t):
        return dict(device_id=(0, n, t), device_id_type=MESH)

    def lon_peer(dz, dy):
        return lax.rem(z + dz, 4) * 4 + lax.rem(y + dy, 4)

    def lat_peer(d):
        return lax.rem(lat + d, LAT)

    def quad(tq):
        return z * 4 + lax.rem(y, 2) + 2 * (tq // 2), (lat // 2) * 2 + tq % 2

    def rows(ch, size=CROWS, off=0):
        return pl.ds(pl.multiple_of(ch * CROWS + off, 16), size)

    lanes_half = pl.ds(pl.multiple_of(half * 128, 128), 128)

    def x_load(tg, ch):
        part = (pl.ds(tg * 4, 4), rows(ch))
        return pltpu.make_async_copy(x_hbm.at[part], xf.at[part], x_sem.at[tg * CHUNKS + ch])

    def start_x(n, _):
        x_load(n // CHUNKS, lax.rem(n, CHUNKS)).start()
        return 0

    bar = pltpu.get_barrier_semaphore()
    for dz, dy in PEERS:
        pl.semaphore_signal(bar, inc=1, **dev(lon_peer(dz, dy), lat))
    for d in range(1, LAT):
        pl.semaphore_signal(bar, inc=1, **dev(lon, lat_peer(d)))
    pl.semaphore_signal(bar, inc=1, **dev(lon_peer(0, 2), (lat // 2) * 2 + 1 - core))

    lax.fori_loop(0, 2 * CHUNKS, start_x, 0)
    fwd_load = pltpu.make_async_copy(ft_hbm.at[:, lat], fs, tab_sem.at[0])
    inv_load = pltpu.make_async_copy(it_hbm.at[:, lat], gs, tab_sem.at[1])
    fwd_load.start()
    inv_load.start()

    def degree(idx):
        return jnp.where(idx < 16, quarter * 16 + idx, (7 - quarter) * 16 + idx - 16)

    def w_load(idx):
        slot = lax.rem(idx, W_SLOTS)
        return pltpu.make_async_copy(w_hbm.at[degree(idx)], ws.at[slot], w_sem.at[slot])

    for idx in range(W_SLOTS):
        w_load(jnp.int32(idx)).start()

    for i in range(2, 16):
        rd[i, 0:16 * (i // 2), :] = jnp.zeros((16 * (i // 2), 256), BF16)

    def convert(tg):
        def body(ch, _):
            x_load(tg, ch).wait()
            for zz in range(4):
                for h in range(2):
                    xs[4 * zz + 2 * h + (zz + tg) % 2, rows(ch), :] = xf[4 * tg + zz, rows(ch), h * 128:(h + 1) * 128].astype(BF16)
            return 0

        lax.fori_loop(0, CHUNKS, body, 0)

    def send_a(tg):
        shift = lax.rem(group + tg, 2)

        def body(ch, _):
            for dz, dy in EVEN:
                peer = lon_peer(dz, dy + shift)
                src, dst = xs.at[peer, rows(ch)], ra.at[lon, rows(ch)]

                def remote():
                    pltpu.make_async_remote_copy(src, dst, a_send.at[ch], a_recv.at[ch], **dev(peer, lat)).start()

                if (dz, dy) != (0, 0):
                    remote()
                else:
                    pl.when(shift != 0)(remote)

                    @pl.when(shift == 0)
                    def _():
                        pltpu.make_async_copy(src, dst, a_recv.at[ch]).start()
            return 0

        lax.fori_loop(0, CHUNKS, body, 0)

    convert(0)
    pl.semaphore_wait(bar, 15 + 7 + 1)
    send_a(0)
    convert(1)
    send_a(1)

    fwd_load.wait()
    inv_load.wait()

    def prep_tables(i, _):
        fb[i] = fs[i].T.astype(BF16)
        ib[i] = gs[i].astype(BF16)
        return 0

    lax.fori_loop(0, 16, prep_tables, 0)

    def prep_weights(idx, _):
        w_load(idx).wait()
        slot = lax.rem(idx, W_SLOTS)
        for ri in range(2):
            for it in range(2):
                wb[idx, :, ri * 256 + it * 128: ri * 256 + (it + 1) * 128] = ws[slot, pl.ds(2 * it + ri, 256, stride=4), :].astype(BF16)

        @pl.when(idx + W_SLOTS < 32)
        def _():
            w_load(idx + W_SLOTS).start()

        return 0

    def take_b(ch):
        chunk = pl.ds(ch * CHUNK_T, CHUNK_T)
        pltpu.make_async_copy(rb.at[:, chunk], rb.at[:, chunk], b_recv.at[ch]).wait()

        def one(kk, _):
            for tt in range(CHUNK_T):
                row = pl.multiple_of((kk * 24 + ch * CHUNK_T + tt) * TS, 8)
                t1[pl.ds(row, 32), :] = rb[kk, ch * CHUNK_T + tt].astype(F32)
            return 0

        lax.fori_loop(0, LAT, one, 0)

    def dft(ch, _):
        lax.fori_loop(ch * 3, jnp.minimum(ch * 3 + 3, 32), prep_weights, 0)
        pltpu.make_async_copy(ra.at[:, rows(ch)], ra.at[:, rows(ch)], a_recv.at[ch]).wait()
        out = jnp.dot(dfwd[...], ra[:, rows(ch), :].reshape(768, 128), preferred_element_type=F32)
        sp[:, pl.ds(ch * CHUNK_T, CHUNK_T)] = out.astype(BF16).reshape(8, 2, 32, 128)
        chunk = pl.ds(ch * CHUNK_T, CHUNK_T)
        for d in range(1, LAT):
            peer = lat_peer(d)
            pltpu.make_async_remote_copy(sp.at[peer, chunk], rb.at[lat, chunk], b_send.at[ch], b_recv.at[ch],
                                         **dev(lon, peer)).start()
        pltpu.make_async_copy(sp.at[lat, chunk], rb.at[lat, chunk], b_recv.at[ch]).start()

        @pl.when(ch > 0)
        def _():
            take_b(ch - 1)

        return 0

    lax.fori_loop(0, CHUNKS, dft, 0)
    take_b(CHUNKS - 1)

    def legendre(i, _):
        rhs = jnp.concatenate([t1[pl.ds(i, 192, stride=TS), :], t1[pl.ds(16 + i, 192, stride=TS), :]], axis=1).astype(BF16)
        cf[i] = jnp.dot(fb[i], rhs, preferred_element_type=F32).astype(BF16)
        return 0

    lax.fori_loop(0, 16, legendre, 0, unroll=4)

    for b in range(7, -1, -1):
        tq, lohi, n = (b, 0, 2 * b + 2) if b < 4 else (7 - b, 1, 2 * b + 2)
        src = cf.at[pl.ds(0, n), pl.ds(16 * b, 16)]
        dst = rc.at[pl.ds((quarter * 2 + lohi) * 16, n)]

        @pl.when(quarter == tq)
        def _():
            pltpu.make_async_copy(src, dst, c_recv.at[lohi]).start()

        @pl.when(quarter != tq)
        def _():
            pltpu.make_async_remote_copy(src, dst, c_send, c_recv.at[lohi], **dev(*quad(tq))).start()

    def take_c(lohi):
        for qq in range(4):
            n = 4 * (2 * qq + 2 if lohi == 0 else 16 - 2 * qq)

            @pl.when(quarter == qq)
            def _():
                pltpu.make_async_copy(rc.at[pl.ds(0, n)], rc.at[pl.ds(0, n)], c_recv.at[lohi]).wait()

        def one(i, _):
            for sq in range(4):
                u = (sq * 2 + lohi) * 16 + i
                for ri in range(2):
                    t2[ri, pl.ds(pl.multiple_of(u * LS, 8), 16), :] = rc[u, :, ri * 128:(ri + 1) * 128].astype(F32)
            return 0

        lax.fori_loop(0, 16, one, 0)

    def mix(idx, lohi):
        r = idx - lohi * 16

        def part(ri):
            return jnp.concatenate([jnp.concatenate([
                t2[ri, pl.ds(((2 * hs + cs) * 2 + lohi) * 16 * LS + r, 16, stride=LS), :] for hs in range(2)], axis=1)
                for cs in range(2)], axis=0)

        re, im = part(0), part(1)
        lhs = jnp.concatenate([jnp.concatenate([re, -im], axis=1), jnp.concatenate([im, re], axis=1)], axis=0).astype(BF16)
        out = lax.dot_general(lhs, wb[idx], (((1,), (1,)), ((), ())), preferred_element_type=F32)
        for ri in range(2):
            for oh in range(2):
                t3[ri * 2 + oh, pl.ds(lohi * 32 * LS + r, 32, stride=LS), :] = out[ri * 32:(ri + 1) * 32, oh * 128:(oh + 1) * 128]

    for lohi in (1, 0):
        take_c(lohi)

        def mix_step(idx, _, lohi=lohi):
            mix(idx, lohi)
            return 0

        lax.fori_loop(lohi * 16, lohi * 16 + 16, mix_step, 0, unroll=4)

        def pack_d(i, _, lohi=lohi):
            for oh in range(2):
                for cs in range(2):
                    for ri in range(2):
                        row = pl.multiple_of(lohi * 32 * LS + (cs * 16 + i) * LS, 8)
                        sd[((oh * 2 + cs) * 2 + lohi) * 16 + i, :, ri * 128:(ri + 1) * 128] = t3[ri * 2 + oh, pl.ds(row, 16), :].astype(BF16)
            return 0

        lax.fori_loop(0, 16, pack_d, 0)

        for qq in range(4):
            b = qq if lohi == 0 else 7 - qq
            n = 2 * b + 2

            @pl.when(quarter == qq)
            def _():
                for tq in range(4):
                    src = sd.at[pl.ds((tq * 2 + lohi) * 16, n)]
                    dst = rd.at[pl.ds(0, n), pl.ds(16 * b, 16)]
                    if tq == qq:
                        pltpu.make_async_copy(src, dst, d_recv).start()
                    else:
                        pltpu.make_async_remote_copy(src, dst, d_send, d_recv, **dev(*quad(tq))).start()

    pltpu.make_async_copy(rc.at[pl.ds(0, 72)], rc.at[pl.ds(0, 72)], d_recv).wait()

    def inverse(i, _):
        out = jnp.dot(ib[i], rd[i], preferred_element_type=F32)
        t1[pl.ds(i, 192, stride=TS), :] = out[:, :128]
        t1[pl.ds(16 + i, 192, stride=TS), :] = out[:, 128:]
        return 0

    lax.fori_loop(0, 16, inverse, 0, unroll=4)

    def send_e(ch, _):
        chunk = pl.ds(ch * CHUNK_T, CHUNK_T)

        def one(kk, _):
            for tt in range(CHUNK_T):
                row = pl.multiple_of((kk * 24 + ch * CHUNK_T + tt) * TS, 8)
                s2[kk, ch * CHUNK_T + tt] = t1[pl.ds(row, 32), :].astype(BF16)
            return 0

        lax.fori_loop(0, LAT, one, 0)
        for d in range(1, LAT):
            peer = lat_peer(d)
            pltpu.make_async_remote_copy(s2.at[peer, chunk], rebuf.at[lat, chunk], e_send.at[ch], e_recv.at[ch],
                                         **dev(lon, peer)).start()
        pltpu.make_async_copy(s2.at[lat, chunk], rebuf.at[lat, chunk], e_recv.at[ch]).start()
        return 0

    lax.fori_loop(0, CHUNKS, send_e, 0)

    def idft(ch, _):
        chunk = pl.ds(ch * CHUNK_T, CHUNK_T)
        pltpu.make_async_copy(rebuf.at[:, chunk], rebuf.at[:, chunk], e_recv.at[ch]).wait()
        out = jnp.dot(dinv[...], rebuf[:, chunk].reshape(512, 128), preferred_element_type=F32)
        ys[:, rows(ch), :] = out.astype(BF16).reshape(16, 48, 128)
        arrived = f_recv.at[group * CHUNKS + ch]
        for dz, dy in PEERS:
            peer = lon_peer(dz, dy)
            pltpu.make_async_remote_copy(ys.at[peer, rows(ch)], yr.at[sample, rows(ch), lanes_half], f_send, arrived,
                                         **dev(peer, lat)).start()
        pltpu.make_async_copy(ys.at[lon, rows(ch)], yr.at[sample, rows(ch), lanes_half], arrived).start()
        return 0

    lax.fori_loop(0, CHUNKS, idft, 0)

    def finish_rows(n, _):
        tg, ch = n // CHUNKS, lax.rem(n, CHUNKS)
        part = (pl.ds(tg * 4, 4), rows(ch))
        pltpu.make_async_copy(yr.at[part], yr.at[part], f_recv.at[n]).wait()
        for k in range(4):
            xf[tg * 4 + k, rows(ch), :] += jax.nn.gelu(yr[tg * 4 + k, rows(ch), :].astype(F32), approximate=True)
        pltpu.make_async_copy(xf.at[part], o_hbm.at[part], o_sem).start()
        return 0

    lax.fori_loop(0, 2 * CHUNKS, finish_rows, 0)

    def drain(ch, _):
        chunk = pl.ds(ch * CHUNK_T, CHUNK_T)
        pltpu.make_async_copy(xs.at[pl.ds(0, 15), rows(ch)], xs.at[pl.ds(0, 15), rows(ch)], a_send.at[ch]).wait()
        pltpu.make_async_copy(sp.at[pl.ds(0, 7), chunk], sp.at[pl.ds(0, 7), chunk], b_send.at[ch]).wait()
        pltpu.make_async_copy(s2.at[pl.ds(0, 7), chunk], s2.at[pl.ds(0, 7), chunk], e_send.at[ch]).wait()
        return 0

    lax.fori_loop(0, CHUNKS, drain, 0)
    for tq in range(4):
        @pl.when(quarter == tq)
        def _():
            n = 72 - 18
            pltpu.make_async_copy(rc.at[pl.ds(0, n)], rc.at[pl.ds(0, n)], c_send).wait()
            pltpu.make_async_copy(rc.at[pl.ds(0, n)], rc.at[pl.ds(0, n)], d_send).wait()
    pltpu.make_async_copy(ys.at[pl.ds(0, 15)], ys.at[pl.ds(0, 15)], f_send).wait()
    pltpu.make_async_copy(xf, o_hbm, o_sem).wait()


def solution(mesh):
    grid_spec = P('member', None, 'lat', 'lon')
    dfwd, dinv = dft_matrices()

    def local_layer(field_in, fwd_table, inv_table, mix_weights):
        rows_view = field_in.transpose(0, 2, 3, 1).reshape(SAMPLES, ROWS, 256)
        ft = fwd_table.transpose(0, 2, 1).reshape(16, 8, 192, 128)
        it = inv_table.transpose(0, 2, 1).reshape(16, 8, 192, 128)
        w = mix_weights.reshape(128, 256, 2, 128, 2).transpose(0, 1, 2, 4, 3).reshape(128, 1024, 128)
        dma = pltpu.SemaphoreType.DMA
        out = pl.pallas_call(
            kernel,
            out_shape=jax.ShapeDtypeStruct((SAMPLES, ROWS, 256), F32),
            in_specs=[pl.BlockSpec(memory_space=pl.ANY)] * 4 + [pl.BlockSpec(memory_space=pltpu.VMEM)] * 2,
            out_specs=pl.BlockSpec(memory_space=pl.ANY),
            scratch_shapes=[
                pltpu.VMEM((SAMPLES, ROWS, 256), F32),
                pltpu.VMEM((LON, ROWS, 128), BF16),
                pltpu.VMEM((LON, ROWS, 128), BF16),
                pltpu.VMEM((LAT, 24, 32, 128), BF16),
                pltpu.VMEM((LAT, 24, 32, 128), BF16),
                pltpu.VMEM((192 * TS, 128), F32),
                pltpu.VMEM((16, 128, 256), BF16),
                pltpu.VMEM((128, 16, 256), BF16),
                pltpu.VMEM((2, 128 * LS, 128), F32),
                pltpu.VMEM((32, 256, 512), BF16),
                pltpu.VMEM((W_SLOTS, 1024, 128), F32),
                pltpu.VMEM((16, 192, 128), F32),
                pltpu.VMEM((16, 192, 128), F32),
                pltpu.VMEM((16, 128, 192), BF16),
                pltpu.VMEM((16, 192, 128), BF16),
                pltpu.VMEM((4, 64 * LS, 128), F32),
                pltpu.VMEM((128, 16, 256), BF16),
                pltpu.VMEM((16, 128, 256), BF16),
                pltpu.VMEM((LAT, 24, 32, 128), BF16),
                pltpu.VMEM((LAT, 24, 32, 128), BF16),
                pltpu.VMEM((LON, ROWS, 128), BF16),
                pltpu.VMEM((SAMPLES, ROWS, 256), BF16),
                dma((2 * CHUNKS,)), dma((2,)), dma((W_SLOTS,)),
                dma((CHUNKS,)), dma((CHUNKS,)), dma((CHUNKS,)), dma((CHUNKS,)),
                dma, dma((2,)), dma, dma,
                dma((CHUNKS,)), dma((CHUNKS,)), dma, dma((2 * CHUNKS,)), dma,
            ],
            compiler_params=pltpu.CompilerParams(collective_id=0, has_side_effects=True, vmem_limit_bytes=67043328),
        )(rows_view, ft, it, w, jnp.asarray(dfwd), jnp.asarray(dinv))
        return out.reshape(SAMPLES, 24, 24, 256).transpose(0, 3, 1, 2)

    return jax.shard_map(local_layer, mesh=mesh, in_specs=(grid_spec, P(), P(), P()), out_specs=grid_spec, check_vma=False)
```

```python
import math
import numpy as np
import jax
import jax.numpy as jnp
from jax import lax
from jax.experimental import pallas as pl
from jax.experimental.pallas import tpu as pltpu
from jax.sharding import PartitionSpec as P

MESH = pl.DeviceIdType.MESH
F32 = jnp.float32
BF16 = jnp.bfloat16

SAMPLES = 8
LON = 16
LAT = 8
ROWS = 576
CHUNKS = 6
TS = 40
LS = 24
W_SLOTS = 8
GRID = (2, LON, 288, 128)
SPEC = (2, LAT, 12, 32, 128)
A1_EARLY = 4

FAR = sorted(((dz, dy) for dz in range(4) for dy in range(4)), key=lambda d: -min(d[0], 4 - d[0]) - min(d[1], 4 - d[1]))
PEERS = FAR[:-1]


def dft_matrices():
    lon_ids = np.arange(384)
    waves = np.arange(128)
    phase = np.float32(2.0 * math.pi / 384) * ((lon_ids[:, None] * waves[None, :]) % 384).astype(np.float32)
    cos_val, sin_val = np.cos(phase), np.sin(phase)
    weight = np.where(waves == 0, 1.0, 2.0).astype(np.float32)
    fwd = np.stack([cos_val, -sin_val])
    inv = np.stack([weight * cos_val, -weight * sin_val])
    out = []
    for tab in (fwd, inv):
        tab = tab.reshape(2, 16, 24, 16, 8)
        full = np.zeros((8, 2, 2, 16, 16, 2, 24), np.float32)
        part = tab.transpose(4, 0, 3, 1, 2)
        for tt in range(2):
            full[:, tt, :, :, :, tt, :] = part
        out.append(full.reshape(512, 768))
    return out[0].astype(jnp.bfloat16), np.ascontiguousarray(out[1].T).astype(jnp.bfloat16)


def kernel(x_hbm, ft_hbm, it_hbm, w_hbm, dfwd_hbm, dinv_hbm, o_hbm,
           xf, xs, ra, sp, rb, t1, cf, rc, t2, wb, ws, fs, gs, fb, ib, t3, sd, rd, s2, rebuf, ys, yr, dfwd, dinv,
           x_sem, tab_sem, w_sem, a_send, a_recv, b_send, b_recv, c_send, c_recv, d_send, d_recv,
           e_send, e_recv, f_send, f_recv, o_sem):
    lon = lax.axis_index('lon')
    lat = lax.axis_index('lat')
    z, y = lon // 4, lax.rem(lon, 4)
    core = lax.rem(lat, 2)
    block = jnp.where(core == 0, y, 7 - y)

    def dev(n, t):
        return dict(device_id=(0, n, t), device_id_type=MESH)

    def lon_peer(dz, dy):
        return lax.rem(z + dz, 4) * 4 + lax.rem(y + dy, 4)

    def lat_peer(d):
        return lax.rem(lat + d, LAT)

    def mixer(tq, tc):
        return dev(z * 4 + tq, (lat // 2) * 2 + tc)

    def wide(ch):
        return pl.ds(pl.multiple_of(ch * 96, 16), 96)

    def rows(ch):
        return pl.ds(pl.multiple_of(ch * 48, 16), 48)

    def pair(ch):
        return pl.ds(ch * 2, 2)

    def await_copy(ref, sem):
        pltpu.make_async_copy(ref, ref, sem).wait()

    def swap(a, b):
        low = lax.broadcasted_iota(jnp.int32, a.shape, 1) < 64
        return jnp.where(low, a, pltpu.roll(b, 64, 1)), jnp.where(low, pltpu.roll(a, 64, 1), b)

    bar = pltpu.get_barrier_semaphore()
    for dz, dy in PEERS:
        pl.semaphore_signal(bar, inc=1, **dev(lon_peer(dz, dy), lat))
    for d in range(1, LAT):
        pl.semaphore_signal(bar, inc=1, **dev(lon, lat_peer(d)))
    for dy in range(1, 4):
        pl.semaphore_signal(bar, inc=1, **dev(lon_peer(0, dy), (lat // 2) * 2 + 1 - core))

    def x_load(g, ch):
        part = (pl.ds(4 * g, 4), wide(ch))
        return pltpu.make_async_copy(x_hbm.at[part], xf.at[part], x_sem.at[g, ch])

    for g in range(2):
        for ch in range(CHUNKS):
            x_load(g, ch).start()
    fwd_load = pltpu.make_async_copy(ft_hbm.at[:, lat], fs, tab_sem.at[0])
    inv_load = pltpu.make_async_copy(it_hbm.at[:, lat], gs, tab_sem.at[1])
    dfwd_load = pltpu.make_async_copy(dfwd_hbm, dfwd, tab_sem.at[2])
    dinv_load = pltpu.make_async_copy(dinv_hbm, dinv, tab_sem.at[3])
    dfwd_load.start()
    fwd_load.start()
    inv_load.start()

    def w_load(idx):
        slot = lax.rem(idx, W_SLOTS)
        return pltpu.make_async_copy(w_hbm.at[block * 16 + idx], ws.at[slot], w_sem.at[slot])

    for idx in range(W_SLOTS):
        w_load(jnp.int32(idx)).start()
    dinv_load.start()

    for g in range(2):
        for i in range(2, 16):
            rd[g, i, 0:16 * (i // 2), :] = jnp.zeros((16 * (i // 2), 128), BF16)

    def convert(g, ch):
        x_load(g, ch).wait()
        for s in range(4):
            for it in range(2):
                lanes = slice(it * 128, (it + 1) * 128)
                parts = [swap(xf[4 * g + s, pl.ds(pl.multiple_of(ch * 96 + tp * 48, 8), 24), lanes],
                              xf[4 * g + s, pl.ds(pl.multiple_of(ch * 96 + tp * 48 + 24, 8), 24), lanes]) for tp in range(2)]
                for odd in range(2):
                    xs[g, 4 * s + 2 * it + odd, rows(ch), :] = jnp.concatenate([parts[0][odd], parts[1][odd]], axis=0).astype(BF16)

    def send_a(g, ch):
        for dz, dy in PEERS:
            peer = lon_peer(dz, dy)
            pltpu.make_async_remote_copy(xs.at[g, peer, rows(ch)], ra.at[g, lon, rows(ch)], a_send.at[g], a_recv.at[g, ch],
                                         **dev(peer, lat)).start()
        pltpu.make_async_copy(xs.at[g, lon, rows(ch)], ra.at[g, lon, rows(ch)], a_recv.at[g, ch]).start()

    def loop(fun, g, start=0, stop=CHUNKS):
        def step(ch, _):
            fun(g, ch)
            return 0

        lax.fori_loop(start, stop, step, 0)

    def convert_send(g, ch):
        convert(g, ch)
        send_a(g, ch)

    pl.semaphore_wait(bar, 15 + 7 + 3)
    loop(convert_send, 0)
    loop(convert_send, 1, 0, A1_EARLY)
    loop(convert, 1, A1_EARLY)

    fwd_load.wait()
    inv_load.wait()

    def prep_tables(i, _):
        fb[i] = jnp.concatenate([fs[i, pl.ds(tt, 96, stride=2), :] for tt in range(2)], axis=0).T.astype(BF16)
        ib[i] = jnp.concatenate([gs[i, pl.ds(tt, 96, stride=2), :] for tt in range(2)], axis=0).astype(BF16)
        return 0

    lax.fori_loop(0, 16, prep_tables, 0)

    def prep_weights(idx, _):
        w_load(idx).wait()
        slot = lax.rem(idx, W_SLOTS)
        for it in range(2):
            both = swap(ws[slot, pl.ds(2 * it, 256, stride=4), :], ws[slot, pl.ds(2 * it + 1, 256, stride=4), :])
            for odd in range(2):
                wb[idx, :, (2 * it + odd) * 128:(2 * it + odd + 1) * 128] = both[odd].astype(BF16)

        @pl.when(idx + W_SLOTS < 16)
        def _():
            w_load(idx + W_SLOTS).start()

        return 0

    def take_b(g, ch):
        await_copy(rb.at[g, :, pair(ch)], b_recv.at[g, ch])

        def one(kk, _):
            for tp in range(2):
                t1[g, pl.ds(pl.multiple_of((kk * 12 + ch * 2 + tp) * TS, 8), 32), :] = rb[g, kk, ch * 2 + tp].astype(F32)
            return 0

        lax.fori_loop(0, LAT, one, 0)

    def dft(g, ch):
        if g == 0:
            lax.fori_loop(ch * 3, jnp.minimum(ch * 3 + 3, 16), prep_weights, 0)
        await_copy(ra.at[g, :, rows(ch)], a_recv.at[g, ch])
        out = jnp.dot(dfwd[...], ra[g, :, rows(ch), :].reshape(768, 128), preferred_element_type=F32)
        sp[g, :, pair(ch)] = out.astype(BF16).reshape(8, 2, 32, 128)
        for d in range(1, LAT):
            peer = lat_peer(d)
            pltpu.make_async_remote_copy(sp.at[g, peer, pair(ch)], rb.at[g, lat, pair(ch)], b_send.at[g], b_recv.at[g, ch],
                                         **dev(lon, peer)).start()
        pltpu.make_async_copy(sp.at[g, lat, pair(ch)], rb.at[g, lat, pair(ch)], b_recv.at[g, ch]).start()

    def legendre(g):
        def step(i, _):
            rhs = jnp.concatenate(swap(t1[g, pl.ds(i, 96, stride=TS), :], t1[g, pl.ds(16 + i, 96, stride=TS), :]), axis=0).astype(BF16)
            cf[g, i] = jnp.dot(fb[i], rhs, preferred_element_type=F32).astype(BF16)
            return 0

        lax.fori_loop(0, 16, step, 0, unroll=4)

    def send_c(g):
        for b in range(7, -1, -1):
            tq, tc = (b, 0) if b < 4 else (7 - b, 1)
            n = 2 * b + 2
            src = cf.at[g, pl.ds(0, n), pl.ds(16 * b, 16)]
            dst = rc.at[g, pl.ds((y * 2 + core) * 16, n)]

            @pl.when(block == b)
            def _():
                pltpu.make_async_copy(src, dst, c_recv.at[g]).start()

            @pl.when(block != b)
            def _():
                pltpu.make_async_remote_copy(src, dst, c_send.at[g], c_recv.at[g], **mixer(tq, tc)).start()

    def mix(g):
        for b in range(8):
            @pl.when(block == b)
            def _():
                await_copy(rc.at[g, pl.ds(0, 16 * (b + 1))], c_recv.at[g])

        def take_c(i, _):
            for sq in range(8):
                t2[pl.ds(pl.multiple_of((sq * 16 + i) * LS, 8), 16), :] = rc[g, sq * 16 + i].astype(F32)
            return 0

        lax.fori_loop(0, 16, take_c, 0)

        def step(r, _):
            straight, crossed = [], []
            for cs in range(2):
                part = [t2[pl.ds((2 * q + cs) * 16 * LS + r, 16, stride=LS), :] for q in range(4)]
                low = lax.broadcasted_iota(jnp.int32, (16, 128), 1) < 64
                straight.append(jnp.concatenate([jnp.where(low, p, -p) for p in part], axis=1))
                crossed.append(jnp.concatenate([pltpu.roll(p, 64, 1) for p in part], axis=1))
            lhs = jnp.concatenate(straight + crossed, axis=0).astype(BF16)
            out = lax.dot_general(lhs, wb[r], (((1,), (1,)), ((), ())), preferred_element_type=F32)
            for it in range(2):
                both = swap(out[:32, it * 128:(it + 1) * 128], out[32:, it * 128:(it + 1) * 128])
                for odd in range(2):
                    t3[2 * it + odd, pl.ds(r, 32, stride=LS), :] = both[odd]
            return 0

        lax.fori_loop(0, 16, step, 0, unroll=8)

        def pack(i, _):
            for tq in range(4):
                for tc in range(2):
                    sd[g, (tq * 2 + tc) * 16 + i] = t3[tq, pl.ds(pl.multiple_of((tc * 16 + i) * LS, 8), 16), :].astype(BF16)
            return 0

        lax.fori_loop(0, 16, pack, 0)
        for b in range(8):
            n = 2 * b + 2
            own = (b, 0) if b < 4 else (7 - b, 1)

            @pl.when(block == b)
            def _():
                for tq in range(4):
                    for tc in range(2):
                        src = sd.at[g, pl.ds((tq * 2 + tc) * 16, n)]
                        dst = rd.at[g, pl.ds(0, n), pl.ds(16 * b, 16)]
                        if (tq, tc) == own:
                            pltpu.make_async_copy(src, dst, d_recv.at[g]).start()
                        else:
                            pltpu.make_async_remote_copy(src, dst, d_send.at[g], d_recv.at[g], **mixer(tq, tc)).start()

    def inverse(g):
        await_copy(rc.at[g, pl.ds(0, 72)], d_recv.at[g])

        def step(i, _):
            out = jnp.dot(ib[i], rd[g, i], preferred_element_type=F32)
            both = swap(out[:96], out[96:])
            for ri in range(2):
                t1[g, pl.ds(ri * 16 + i, 96, stride=TS), :] = both[ri]
            return 0

        lax.fori_loop(0, 16, step, 0, unroll=4)

    def send_e(g, ch):
        def one(kk, _):
            for tp in range(2):
                s2[g, kk, ch * 2 + tp] = t1[g, pl.ds(pl.multiple_of((kk * 12 + ch * 2 + tp) * TS, 8), 32), :].astype(BF16)
            return 0

        lax.fori_loop(0, LAT, one, 0)
        for d in range(1, LAT):
            peer = lat_peer(d)
            pltpu.make_async_remote_copy(s2.at[g, peer, pair(ch)], rebuf.at[g, lat, pair(ch)], e_send.at[g], e_recv.at[g, ch],
                                         **dev(lon, peer)).start()
        pltpu.make_async_copy(s2.at[g, lat, pair(ch)], rebuf.at[g, lat, pair(ch)], e_recv.at[g, ch]).start()

    def idft(g, ch):
        await_copy(rebuf.at[g, :, pair(ch)], e_recv.at[g, ch])
        out = jnp.dot(dinv[...], rebuf[g, :, pair(ch)].reshape(512, 128), preferred_element_type=F32)
        ys[g, :, rows(ch), :] = out.astype(BF16).reshape(16, 48, 128)
        for dz, dy in PEERS:
            peer = lon_peer(dz, dy)
            pltpu.make_async_remote_copy(ys.at[g, peer, rows(ch)], yr.at[g, lon, rows(ch)], f_send.at[g], f_recv.at[g, ch],
                                         **dev(peer, lat)).start()
        pltpu.make_async_copy(ys.at[g, lon, rows(ch)], yr.at[g, lon, rows(ch)], f_recv.at[g, ch]).start()

    def finish_rows(g, ch):
        await_copy(yr.at[g, :, rows(ch)], f_recv.at[g, ch])
        for s in range(4):
            for it in range(2):
                both = swap(yr[g, 4 * s + 2 * it, rows(ch), :].astype(F32), yr[g, 4 * s + 2 * it + 1, rows(ch), :].astype(F32))
                for tt in range(2):
                    val = jax.nn.gelu(both[tt], approximate=True)
                    for tp in range(2):
                        at = pl.ds(pl.multiple_of(ch * 96 + tp * 48 + tt * 24, 8), 24)
                        xf[4 * g + s, at, it * 128:(it + 1) * 128] += val[tp * 24:(tp + 1) * 24]
        part = (pl.ds(4 * g, 4), wide(ch))
        pltpu.make_async_copy(xf.at[part], o_hbm.at[part], o_sem).start()

    dfwd_load.wait()
    loop(dft, 0)
    loop(take_b, 0)
    legendre(0)
    send_c(0)
    loop(send_a, 1, A1_EARLY)
    loop(dft, 1, 0, 3)
    mix(0)
    loop(dft, 1, 3)
    inverse(0)
    loop(send_e, 0, 0, 3)
    loop(take_b, 1)
    legendre(1)
    send_c(1)
    loop(send_e, 0, 3)
    dinv_load.wait()
    loop(idft, 0, 0, 2)
    mix(1)
    loop(idft, 0, 2)
    inverse(1)
    loop(send_e, 1)
    loop(idft, 1)
    loop(finish_rows, 0)
    loop(finish_rows, 1)

    for g in range(2):
        await_copy(xs.at[g, pl.ds(0, 15)], a_send.at[g])
        await_copy(sp.at[g, pl.ds(0, 7)], b_send.at[g])
        await_copy(s2.at[g, pl.ds(0, 7)], e_send.at[g])
        await_copy(ys.at[g, pl.ds(0, 15)], f_send.at[g])
        for b in range(8):
            @pl.when(block == b)
            def _():
                await_copy(rc.at[g, pl.ds(0, 70 - 2 * b)], c_send.at[g])
                await_copy(rc.at[g, pl.ds(0, 14 * (b + 1))], d_send.at[g])
    pltpu.make_async_copy(xf, o_hbm, o_sem).wait()


def solution(mesh):
    grid_spec = P('member', None, 'lat', 'lon')
    dfwd, dinv = dft_matrices()

    def local_layer(field_in, fwd_table, inv_table, mix_weights):
        rows_view = field_in.transpose(0, 2, 3, 1).reshape(SAMPLES, ROWS, 256)
        ft = fwd_table.transpose(0, 2, 1).reshape(16, 8, 192, 128)
        it = inv_table.transpose(0, 2, 1).reshape(16, 8, 192, 128)
        w = mix_weights.reshape(128, 256, 2, 128, 2).transpose(0, 1, 2, 4, 3).reshape(128, 1024, 128)
        dma = pltpu.SemaphoreType.DMA
        out = pl.pallas_call(
            kernel,
            out_shape=pltpu.VMEM((SAMPLES, ROWS, 256), F32),
            in_specs=[pl.BlockSpec(memory_space=pl.ANY)] * 6,
            out_specs=pl.BlockSpec(memory_space=pl.ANY),
            scratch_shapes=[
                pltpu.VMEM((SAMPLES, ROWS, 256), F32),
                pltpu.VMEM(GRID, BF16),
                pltpu.VMEM(GRID, BF16),
                pltpu.VMEM(SPEC, BF16),
                pltpu.VMEM(SPEC, BF16),
                pltpu.VMEM((2, 96 * TS, 128), F32),
                pltpu.VMEM((2, 16, 128, 128), BF16),
                pltpu.VMEM((2, 128, 16, 128), BF16),
                pltpu.VMEM((128 * LS, 128), F32),
                pltpu.VMEM((16, 256, 512), BF16),
                pltpu.VMEM((W_SLOTS, 1024, 128), F32),
                pltpu.VMEM((16, 192, 128), F32),
                pltpu.VMEM((16, 192, 128), F32),
                pltpu.VMEM((16, 128, 192), BF16),
                pltpu.VMEM((16, 192, 128), BF16),
                pltpu.VMEM((4, 32 * LS, 128), F32),
                pltpu.VMEM((2, 128, 16, 128), BF16),
                pltpu.VMEM((2, 16, 128, 128), BF16),
                pltpu.VMEM(SPEC, BF16),
                pltpu.VMEM(SPEC, BF16),
                pltpu.VMEM(GRID, BF16),
                pltpu.VMEM(GRID, BF16),
                pltpu.VMEM((512, 768), BF16),
                pltpu.VMEM((768, 512), BF16),
                dma((2, CHUNKS)), dma((4,)), dma((W_SLOTS,)),
                dma((2,)), dma((2, CHUNKS)), dma((2,)), dma((2, CHUNKS)),
                dma((2,)), dma((2,)), dma((2,)), dma((2,)),
                dma((2,)), dma((2, CHUNKS)), dma((2,)), dma((2, CHUNKS)), dma,
            ],
            compiler_params=pltpu.CompilerParams(collective_id=0, has_side_effects=True, vmem_limit_bytes=56 * 2**20),
        )(rows_view, ft, it, w, jnp.asarray(dfwd), jnp.asarray(dinv))
        return out.reshape(SAMPLES, 24, 24, 256).transpose(0, 3, 1, 2)

    return jax.shard_map(local_layer, mesh=mesh, in_specs=(grid_spec, P(), P(), P()), out_specs=grid_spec, check_vma=False)
```
